32 devices in a mesh: layer: 4 (over y, x), latent: 8 (over z, core).
Axes of the slice: x: 2, y: 2, z: 4, core: 2. Of those that a mesh axis runs over, the one named last changes fastest.
Arguments:
- tokens: bfloat16 [128, 16384], P('latent', 'layer'), may hold values from -6 to 6
- encoder_weight: bfloat16 [16384, 16384], P('layer', 'latent'), may hold values from -0.046875 to 0.046875
- encoder_bias: float32 [16384], P('latent'), may hold values from -3 to 3, as said below
- decoder_weight: bfloat16 [16384, 16384], P('latent', 'layer'), may hold values from -2 to 2
- decoder_bias: float32 [16384], P('layer'), may hold values from -12 to 12
Outputs:
- encoder_grad: bfloat16 [16384, 16384], P('layer', 'latent')
- decoder_grad: bfloat16 [16384, 16384], P('latent', 'layer')
The draws below stay inside these ranges and needn't reach their ends.
Inputs may be any that keep to these rules, and one draw needn't show every extreme that they name: `encoder_bias`: mean about -0.5.
All inputs are finite; a program needn't handle non-finite values.
Results may differ from the reference program's by a relative error of at most 0.0059.
Values may be sent and summed in bfloat16 or wider, within the bound.
No kernel may reach another device: no remote copies, remote signals or barrier semaphores. Data moves between devices by JAX's collectives and lax.ppermute only.
A program may use at most 128 MiB of HBM per device.

```python
import jax
import jax.numpy as jnp
from jax import lax

L = 4
D = 4096
F = 16384
TOKENS = 128


def decoder_values(key):
    key_base = jax.random.fold_in(jax.random.fold_in(key, 71), 0)
    key_rows = jax.random.fold_in(jax.random.fold_in(key, 71), 1)
    key_jitter = jax.random.fold_in(jax.random.fold_in(key, 71), 3)
    base_draw = jnp.clip(jax.random.normal(key_base, (F, L, D), jnp.float32), -4.0, 4.0)
    row_scale = jnp.exp(jax.random.uniform(key_rows, (F, L, 1), jnp.float32, jnp.log(0.3), jnp.log(3.0)))
    ramp_scale = jnp.exp(jnp.log(3.0) * jnp.arange(L * D, dtype=jnp.float32) / (L * D - 1.0))
    jitter = jnp.exp(jax.random.uniform(key_jitter, (L * D,), jnp.float32, jnp.log(0.7), jnp.log(1.4)))
    col_scale = (ramp_scale * jitter)[None, :] / 1.5
    values = (base_draw * row_scale).reshape(F, L * D) * col_scale / jnp.sqrt(F * 1.0)
    return values.astype(jnp.bfloat16)


def latent_bias_values(key):
    standard = jax.random.normal(jax.random.fold_in(key, 53), (F,), jnp.float32)
    return jnp.clip(0.5 * standard - 0.5, -3.0, 3.0)


def draw_decoder_weight(key, part):
    return decoder_values(key)


def draw_encoder_bias(key, part):
    return latent_bias_values(key)


def draw_decoder_bias(key, part):
    latent_bias = latent_bias_values(key)
    grid_points = jnp.linspace(-7.0, 7.0, 561).astype(jnp.float32)
    density = jnp.exp(-0.5 * grid_points * grid_points)
    density = density / jnp.sum(density)
    smoothed = jax.nn.softplus(4.0 * (latent_bias[:, None] + grid_points[None, :])) / 4.0
    expected = jnp.dot(smoothed, density, precision=lax.Precision.HIGHEST)
    decoder = decoder_values(key).astype(jnp.float32)
    offset = jnp.dot(expected, decoder, precision=lax.Precision.HIGHEST)
    jitter_term = 0.03 * jax.random.normal(jax.random.fold_in(key, 97), (L * D,), jnp.float32)
    return jnp.clip(jitter_term - offset, -12.0, 12.0)


def block_levels(rng, extent, cuts, low, top_value):
    level, own = 1.0, jax.random.fold_in(rng, 6)
    for dim, parts in cuts:
        steps = jnp.exp(jax.random.uniform(jax.random.fold_in(own, dim), (parts,), jnp.float32, low / len(cuts), top_value / len(cuts)))
        level = level * jnp.repeat(steps, extent[dim] // parts).reshape([-1 if axis == dim else 1 for axis in range(len(extent))])
    return level


def normal_values(key, shape, width, limit, shards=(), held_as=jnp.bfloat16):
    result = jax.random.normal(key, shape, jnp.float32) * width
    if len(shards) > 0:
        result = block_levels(key, shape, shards, -0.22, 0.18) * result
    return jnp.clip(result, min=-limit, max=limit).astype(held_as)


def setup_inputs(seed: int = 0) -> dict:
    streams_of = jax.random.split(jax.random.key(seed), 6)
    tokens = normal_values(streams_of[0], (TOKENS, L * D), 1.0, 6.0, ((0, 8), (1, 4)))
    encoder_weight = normal_values(streams_of[1], (L * D, F), (L * D) ** -0.5, 0.046875, ((0, 4), (1, 8)))
    encoder_bias = draw_encoder_bias(jax.random.fold_in(streams_of[5], 71), 0)
    decoder_weight = draw_decoder_weight(jax.random.fold_in(streams_of[5], 71), 0)
    decoder_bias = draw_decoder_bias(jax.random.fold_in(streams_of[5], 71), 0)
    return {"tokens": tokens, "encoder_weight": encoder_weight, "encoder_bias": encoder_bias, "decoder_weight": decoder_weight, "decoder_bias": decoder_bias}


LOSS_SCALE = 0.0625
SPARSITY = 0.5
sharpness = 4.0
epsilon = 1e-06

def reference(tokens, encoder_weight, encoder_bias, decoder_weight, decoder_bias):
    preact = jnp.dot(tokens, encoder_weight, preferred_element_type=jnp.float32) + encoder_bias
    hidden = (jax.nn.softplus(sharpness * preact) / sharpness).astype(jnp.bfloat16)
    slopes = jax.nn.sigmoid(sharpness * preact)
    wide = decoder_weight.astype(jnp.float32).reshape(F, L, D)
    row_norms = jnp.sqrt(lax.optimization_barrier(jnp.sum(wide * wide, axis=2)) + epsilon)
    weights_sum = lax.optimization_barrier(jnp.sum(row_norms, axis=1))
    errors = jnp.dot(hidden, decoder_weight, preferred_element_type=jnp.float32) + decoder_bias - tokens.astype(jnp.float32)
    error_grad = (LOSS_SCALE * errors).astype(jnp.bfloat16)
    hidden_grad = lax.dot_general(error_grad, decoder_weight, (((1,), (1,)), ((), ())), preferred_element_type=jnp.float32)
    hidden_grad = hidden_grad + LOSS_SCALE * SPARSITY * weights_sum[None, :]
    pre_grad = (hidden_grad * slopes).astype(jnp.bfloat16)
    encoder_grad = lax.dot_general(tokens, pre_grad, (((0,), (0,)), ((), ())), preferred_element_type=jnp.float32).astype(jnp.bfloat16)
    totals = lax.optimization_barrier(jnp.sum(hidden.astype(jnp.float32), axis=0))
    direct = lax.dot_general(hidden, error_grad, (((0,), (0,)), ((), ())), preferred_element_type=jnp.float32)
    sparse_term = (wide / row_norms[:, :, None]).reshape(F, L * D) * (LOSS_SCALE * SPARSITY * totals[:, None])
    decoder_grad = (direct + sparse_term).astype(jnp.bfloat16)
    return (encoder_grad, decoder_grad)
```

```python
import functools

import jax
import jax.numpy as jnp
from jax import lax
from jax.experimental import pallas as pl
from jax.experimental.pallas import tpu as pltpu
from jax.sharding import PartitionSpec as P

L = 4
D = 4096


LOSS_SCALE = 0.0625
SPARSITY = 0.5
sharpness = 4.0
epsilon = 1e-06


CHUNKS = 2
F32 = jnp.float32
BF16 = jnp.bfloat16
VMEM_LIMIT = 40 * 1024 * 1024


def general(tokens, encoder_weight, encoder_bias, decoder_weight, decoder_bias):
    rows_dev, width_dev = tokens.shape
    latents_dev = encoder_weight.shape[1]
    groups = lax.axis_size("layer")
    layer_index = lax.axis_index("layer") * width_dev // D
    wide = decoder_weight.astype(jnp.float32)
    squares_own = jnp.sum(wide * wide, axis=1)
    placed = jnp.where(jnp.arange(L)[:, None] == layer_index, squares_own[None, :], 0.0)
    squares = lax.psum(placed, "layer")
    row_norms = jnp.sqrt(squares + epsilon)
    weights_sum = jnp.sum(row_norms, axis=0)
    own_norm = lax.dynamic_slice_in_dim(row_norms, layer_index, 1, 0)[0]
    every_token = lax.all_gather(tokens, "latent", axis=0, tiled=True)
    partial_value = jnp.dot(every_token, encoder_weight, preferred_element_type=jnp.float32)
    share_width = latents_dev // groups
    offset = lax.axis_index("layer") * share_width
    preact = lax.psum_scatter(partial_value, "layer", scatter_dimension=1, tiled=True)
    preact = preact + lax.dynamic_slice_in_dim(encoder_bias, offset, share_width, 0)[None, :]
    hidden_share = (jax.nn.softplus(sharpness * preact) / sharpness).astype(jnp.bfloat16)
    hidden = lax.all_gather(hidden_share, "layer", axis=1, tiled=True)
    slopes = jax.nn.sigmoid(sharpness * preact)
    rebuilt = lax.psum(
        jnp.dot(hidden, decoder_weight, preferred_element_type=jnp.float32), "latent"
    )
    errors = rebuilt + decoder_bias[None, :] - every_token.astype(jnp.float32)
    error_grad = (LOSS_SCALE * errors).astype(jnp.bfloat16)
    back_terms = lax.dot_general(
        error_grad, decoder_weight, (((1,), (1,)), ((), ())), preferred_element_type=jnp.float32
    )
    summed = lax.psum_scatter(back_terms, "layer", scatter_dimension=1, tiled=True)
    penalty = lax.dynamic_slice_in_dim(weights_sum, offset, share_width, 0)
    grad_share = ((summed + LOSS_SCALE * SPARSITY * penalty[None, :]) * slopes).astype(jnp.bfloat16)
    pre_grad = lax.all_gather(grad_share, "layer", axis=1, tiled=True)
    encoder_grad = lax.dot_general(
        every_token, pre_grad, (((0,), (0,)), ((), ())), preferred_element_type=jnp.float32
    ).astype(jnp.bfloat16)
    totals = jnp.sum(hidden.astype(jnp.float32), axis=0)
    direct = lax.dot_general(
        hidden, error_grad, (((0,), (0,)), ((), ())), preferred_element_type=jnp.float32
    )
    sparse_term = wide * (LOSS_SCALE * SPARSITY * totals / own_norm)[:, None]
    decoder_grad = (direct + sparse_term).astype(jnp.bfloat16)
    return (encoder_grad, decoder_grad)


def params(**more):
    return pltpu.CompilerParams(vmem_limit_bytes=VMEM_LIMIT, **more)


def cost(flops, nbytes):
    return pl.CostEstimate(flops=flops, bytes_accessed=nbytes, transcendentals=0)


def product(me, halves, weight, chunk, chunks, groups, acc, extra, transposed):
    half, wide = halves[0].shape
    rows = 2 * half
    share = (weight.shape[0] if transposed else weight.shape[1]) // groups
    last = chunk == chunks - 1
    order = [k for k in range(1, groups)] + [0]

    def body(me_ref, a_ref, b_ref, w_ref, *rest):
        refs = list(rest)
        acc_ref = refs.pop(0) if acc is not None else None
        extra_ref = refs.pop(0) if extra is not None else None
        x = refs.pop()
        step = pl.program_id(0)

        @pl.when(step == 0)
        def _():
            x[:half, :] = a_ref[...]
            x[half:, :] = b_ref[...]

        dims = (((1,), (1,)), ((), ())) if transposed else (((1,), (0,)), ((), ()))
        y = lax.dot_general(x[...], w_ref[...], dims, preferred_element_type=F32)
        if acc_ref is not None:
            y = y + acc_ref[0]
        if extra_ref is not None:
            y = y + extra_ref[...]
        if last:
            for place, k in enumerate(order):
                @pl.when(step == place)
                def _(k=k):
                    refs[k][...] = y.astype(refs[k].dtype)
        else:
            refs[0][0] = y

    def of(step, me_ref):
        k = lax.rem(step + 1, groups)
        return me_ref[0] ^ k

    in_specs = [
        pl.BlockSpec((half, wide), lambda s, m: (0, 0)),
        pl.BlockSpec((half, wide), lambda s, m: (0, 0)),
        pl.BlockSpec((share, wide), lambda s, m: (of(s, m), chunk))
        if transposed
        else pl.BlockSpec((wide, share), lambda s, m: (chunk, of(s, m))),
    ]
    args = [*halves, weight]
    if acc is not None:
        in_specs.append(pl.BlockSpec((1, rows, share), lambda s, m: (s, 0, 0)))
        args.append(acc)
    if extra is not None:
        in_specs.append(pl.BlockSpec((1, share), lambda s, m: (0, of(s, m))))
        args.append(extra)
    if last:
        out_shape = [
            jax.ShapeDtypeStruct((rows, share), F32 if k == 0 else BF16) for k in range(groups)
        ]
        out_specs = [pl.BlockSpec((rows, share), lambda s, m: (0, 0)) for _ in range(groups)]
    else:
        out_shape = [jax.ShapeDtypeStruct((groups, rows, share), F32)]
        out_specs = [pl.BlockSpec((1, rows, share), lambda s, m: (s, 0, 0))]
    out = pl.pallas_call(
        body,
        grid_spec=pltpu.PrefetchScalarGridSpec(
            num_scalar_prefetch=1,
            grid=(groups,),
            in_specs=in_specs,
            out_specs=out_specs,
            scratch_shapes=[pltpu.VMEM((rows, wide), BF16)],
        ),
        out_shape=out_shape,
        compiler_params=params(),
        cost_estimate=cost(2 * rows * wide * share * groups, 2 * wide * share * groups),
        name="back" if transposed else "encode",
    )(me, *args)
    return out if last else out[0]


def rebuild(me, hiddens, weight, chunk, chunks):
    groups = len(hiddens)
    rows, share = hiddens[0].shape
    half = rows // 2
    wide = weight.shape[1] // chunks
    block = min(512, wide)
    steps = wide // block

    def body(me_ref, *refs):
        hidden_refs, weight_refs = refs[:groups], refs[groups : 2 * groups]
        keep, send = refs[2 * groups :]
        y = jnp.dot(hidden_refs[0][...], weight_refs[0][...], preferred_element_type=F32)
        for h, w in zip(hidden_refs[1:], weight_refs[1:]):
            y = y + jnp.dot(h[...], w[...], preferred_element_type=F32)
        keep[...] = y[:half]
        send[...] = y[half:].astype(BF16)

    def weight_spec(k):
        return pl.BlockSpec((share, block), lambda s, m: (m[0] ^ k, chunk * steps + s))

    return pl.pallas_call(
        body,
        grid_spec=pltpu.PrefetchScalarGridSpec(
            num_scalar_prefetch=1,
            grid=(steps,),
            in_specs=[pl.BlockSpec((rows, share), lambda s, m: (0, 0)) for _ in range(groups)]
            + [weight_spec(k) for k in range(groups)],
            out_specs=[pl.BlockSpec((half, block), lambda s, m: (0, s))] * 2,
        ),
        out_shape=[
            jax.ShapeDtypeStruct((half, wide), F32),
            jax.ShapeDtypeStruct((half, wide), BF16),
        ],
        compiler_params=params(),
        cost_estimate=cost(2 * rows * wide * share * groups, 2 * wide * share * groups),
        name="rebuild",
    )(me, *hiddens, *([weight] * groups))


def decoder_gradient(me, hiddens, ks, halves, norm_column, weight, into):
    groups = len(hiddens)
    rows, share = hiddens[0].shape
    half, total = halves[0][0].shape[0], weight.shape[1]
    wide = total // len(halves)
    chunks = len(halves)
    first, count = ks[0], len(ks)

    def body(me_ref, *refs):
        refs = list(refs)
        hidden_refs = [refs.pop(0) for _ in ks]
        error_refs = [(refs.pop(0), refs.pop(0)) for _ in range(chunks)]
        norm_ref, w_ref = refs.pop(0), refs.pop(0)
        if into is not None:
            refs.pop(0)
        out, turned, scale, errors = refs
        k, c = pl.program_id(0), pl.program_id(1)

        @pl.when((k == 0) & (c == 0))
        def _():
            for i, (a, b) in enumerate(error_refs):
                errors[i, :half, :] = a[...]
                errors[i, half:, :] = b[...]

        for i in range(count):
            @pl.when((k == i) & (c == 0))
            def _(i=i):
                h = hidden_refs[i][...].astype(F32).T
                totals = jnp.sum(h, axis=1, keepdims=True)
                turned[...] = h.astype(BF16)
                scale[...] = LOSS_SCALE * SPARSITY * totals / norm_ref[...]

        y = jnp.dot(turned[...], errors[c], preferred_element_type=F32)
        out[...] = (y + w_ref[...].astype(F32) * scale[...]).astype(BF16)

    def of(k, m):
        return m[0] ^ (k + first)

    in_specs = [pl.BlockSpec((rows, share), lambda k, c, m: (0, 0)) for _ in ks]
    args = [hiddens[k] for k in ks]
    for a, b in halves:
        in_specs += [pl.BlockSpec((half, wide), lambda k, c, m: (0, 0))] * 2
        args += [a, b]
    in_specs += [
        pl.BlockSpec((share, 1), lambda k, c, m: (of(k, m), 0)),
        pl.BlockSpec((share, wide), lambda k, c, m: (of(k, m), c)),
    ]
    args += [norm_column, weight]
    aliases = {}
    if into is not None:
        in_specs.append(pl.BlockSpec(memory_space=pl.ANY))
        args.append(into)
        aliases = {len(args): 0}
    return pl.pallas_call(
        body,
        grid_spec=pltpu.PrefetchScalarGridSpec(
            num_scalar_prefetch=1,
            grid=(count, chunks),
            in_specs=in_specs,
            out_specs=pl.BlockSpec((share, wide), lambda k, c, m: (of(k, m), c)),
            scratch_shapes=[
                pltpu.VMEM((share, rows), BF16),
                pltpu.VMEM((share, 1), F32),
                pltpu.VMEM((chunks, rows, wide), BF16),
            ],
        ),
        out_shape=jax.ShapeDtypeStruct(weight.shape, BF16),
        input_output_aliases=aliases,
        compiler_params=params(),
        cost_estimate=cost(4 * rows * total * share * count, 4 * total * share * count),
        name="decoder_gradient",
    )(me, *args)


def encoder_gradient(me, gradients, ks, halves, shape, into):
    rows, share = gradients[0].shape
    chunks = len(halves)
    half, wide = halves[0][0].shape
    first, count = ks[0], len(ks)

    def body(me_ref, *refs):
        refs = list(refs)
        grad_refs = [refs.pop(0) for _ in ks]
        token_refs = [(refs.pop(0), refs.pop(0)) for _ in range(chunks)]
        if into is not None:
            refs.pop(0)
        out, turned = refs
        c, k = pl.program_id(0), pl.program_id(1)

        for i, (a, b) in enumerate(token_refs):
            @pl.when((c == i) & (k == 0))
            def _(a=a, b=b):
                turned[:, :half] = a[...].astype(F32).T.astype(BF16)
                turned[:, half:] = b[...].astype(F32).T.astype(BF16)

        for i in range(count):
            @pl.when(k == i)
            def _(i=i):
                y = jnp.dot(turned[...], grad_refs[i][...], preferred_element_type=F32)
                out[...] = y.astype(BF16)

    in_specs = [pl.BlockSpec((rows, share), lambda c, k, m: (0, 0)) for _ in ks]
    args = [gradients[k] for k in ks]
    for a, b in halves:
        in_specs += [pl.BlockSpec((half, wide), lambda c, k, m: (0, 0))] * 2
        args += [a, b]
    aliases = {}
    if into is not None:
        in_specs.append(pl.BlockSpec(memory_space=pl.ANY))
        args.append(into)
        aliases = {len(args): 0}
    return pl.pallas_call(
        body,
        grid_spec=pltpu.PrefetchScalarGridSpec(
            num_scalar_prefetch=1,
            grid=(chunks, count),
            in_specs=in_specs,
            out_specs=pl.BlockSpec((wide, share), lambda c, k, m: (c, m[0] ^ (k + first))),
            scratch_shapes=[pltpu.VMEM((wide, rows), BF16)],
        ),
        out_shape=jax.ShapeDtypeStruct(shape, BF16),
        input_output_aliases=aliases,
        compiler_params=params(),
        cost_estimate=cost(4 * rows * chunks * wide * share * count, 2 * chunks * wide * share * count),
        name="encoder_gradient",
    )(me, *args)


def shards(tokens, encoder_weight, encoder_bias, decoder_weight, decoder_bias):
    rows_dev, width = tokens.shape
    latents = encoder_weight.shape[1]
    groups = lax.axis_size("layer")
    places = lax.axis_size("latent") // 2
    share = latents // groups
    powers = groups & (groups - 1) == 0 and places & (places - 1) == 0
    if width != D or share % 128 or width % (128 * CHUNKS) or not powers or places < 2:
        return general(tokens, encoder_weight, encoder_bias, decoder_weight, decoder_bias)
    piece = width // CHUNKS
    me = lax.axis_index("layer").astype(jnp.int32).reshape(1)

    def layer_move(x, k):
        return lax.ppermute(x, "layer", [(i, i ^ k) for i in range(groups)])

    def place_move(x, k):
        pairs = [(2 * z + c, 2 * (z ^ k) + c) for z in range(places) for c in range(2)]
        return lax.ppermute(x, "latent", pairs)

    def core_move(x):
        return lax.ppermute(x, "latent", [(i, i ^ 1) for i in range(2 * places)])

    def spread(own):
        mine = jnp.concatenate([own] + [place_move(own, k) for k in range(1, places)], axis=0)
        return mine, core_move(mine)

    def columns(x, c):
        return lax.slice_in_dim(x, c * piece, (c + 1) * piece, axis=x.ndim - 1)

    with jax.named_scope("norms"):
        wide = decoder_weight.astype(F32)
        norms = jnp.sqrt(jnp.sum(wide * wide, axis=1) + epsilon)
        norm_row = (LOSS_SCALE * SPARSITY * norms)[None, :]
        norm_column = norms[:, None]

    with jax.named_scope("tokens"):
        every = [spread(columns(tokens, c)) for c in range(CHUNKS)]
    with jax.named_scope("encode"):
        acc = None
        for c in range(CHUNKS):
            acc = product(me, every[c], encoder_weight, c, CHUNKS, groups, acc, None, False)
    with jax.named_scope("hidden"):
        preact = acc[0]
        for k in range(1, groups):
            preact = preact + layer_move(acc[k], k).astype(F32)
        bias = lax.dynamic_slice_in_dim(encoder_bias, me[0] * share, share, 0)
        preact = preact + bias[None, :]
        hidden = (jax.nn.softplus(sharpness * preact) / sharpness).astype(BF16)
        slopes = jax.nn.sigmoid(sharpness * preact)
        hiddens = [hidden] + [layer_move(hidden, k) for k in range(1, groups)]
    error_grads = []
    back = None
    for c in range(CHUNKS):
        with jax.named_scope(f"errors{c}"):
            keep, send = rebuild(me, hiddens, decoder_weight, c, CHUNKS)
            half = keep + core_move(send).astype(F32)
            parts = [half[k * rows_dev : (k + 1) * rows_dev] for k in range(places)]
            value = parts[0]
            for k in range(1, places):
                value = value + place_move(parts[k].astype(BF16), k).astype(F32)
            value = value + columns(decoder_bias, c)[None, :] - columns(tokens, c).astype(F32)
            error_grads.append(spread((LOSS_SCALE * value).astype(BF16)))
    with jax.named_scope("back"):
        for c in range(CHUNKS):
            extra = norm_row if c == 0 else None
            back = product(
                me, error_grads[c], decoder_weight, c, CHUNKS, groups, back, extra, True
            )
    with jax.named_scope("pre_grad"):
        summed = back[0]
        for k in range(1, groups):
            summed = summed + layer_move(back[k], k).astype(F32)
        grad = (summed * slopes).astype(BF16)
        grads = [grad] + [layer_move(grad, k) for k in range(1, groups)]
    with jax.named_scope("decoder_grad"):
        middle = groups // 2
        decoder_grad = None
        for ks in (list(range(middle)), list(range(middle, groups))):
            decoder_grad = decoder_gradient(
                me, hiddens, ks, error_grads, norm_column, decoder_weight, decoder_grad
            )
    with jax.named_scope("encoder_grad"):
        shape = encoder_weight.shape
        encoder_grad = encoder_gradient(me, grads, [0], every, shape, None)
        encoder_grad = encoder_gradient(
            me, grads, list(range(1, groups)), every, shape, encoder_grad
        )
    return (encoder_grad, decoder_grad)


def solution(mesh):
    placed = (
        P("latent", "layer"),
        P("layer", "latent"),
        P("latent"),
        P("latent", "layer"),
        P("layer"),
    )
    return jax.shard_map(
        shards,
        mesh=mesh,
        in_specs=placed,
        out_specs=(P("layer", "latent"), P("latent", "layer")),
        check_vma=False,
    )
```

```python
import jax
import jax.numpy as jnp
from jax import lax
from jax.experimental import pallas as pl
from jax.experimental.pallas import tpu as pltpu
from jax.sharding import PartitionSpec as P


L = 4
D = 4096


LOSS_SCALE = 0.0625
SPARSITY = 0.5
sharpness = 4.0
epsilon = 1e-06


CHUNKS = 2
F32 = jnp.float32
BF16 = jnp.bfloat16
MIB = 1024 * 1024


def general(tokens, encoder_weight, encoder_bias, decoder_weight, decoder_bias):
    _, width_dev = tokens.shape
    latents_dev = encoder_weight.shape[1]
    groups = lax.axis_size("layer")
    layer_index = lax.axis_index("layer") * width_dev // D
    wide = decoder_weight.astype(jnp.float32)
    squares_own = jnp.sum(wide * wide, axis=1)
    placed = jnp.where(jnp.arange(L)[:, None] == layer_index, squares_own[None, :], 0.0)
    squares = lax.psum(placed, "layer")
    row_norms = jnp.sqrt(squares + epsilon)
    weights_sum = jnp.sum(row_norms, axis=0)
    own_norm = lax.dynamic_slice_in_dim(row_norms, layer_index, 1, 0)[0]
    every_token = lax.all_gather(tokens, "latent", axis=0, tiled=True)
    partial_value = jnp.dot(every_token, encoder_weight, preferred_element_type=jnp.float32)
    share_width = latents_dev // groups
    offset = lax.axis_index("layer") * share_width
    preact = lax.psum_scatter(partial_value, "layer", scatter_dimension=1, tiled=True)
    preact = preact + lax.dynamic_slice_in_dim(encoder_bias, offset, share_width, 0)[None, :]
    hidden_share = (jax.nn.softplus(sharpness * preact) / sharpness).astype(jnp.bfloat16)
    hidden = lax.all_gather(hidden_share, "layer", axis=1, tiled=True)
    slopes = jax.nn.sigmoid(sharpness * preact)
    rebuilt = lax.psum(
        jnp.dot(hidden, decoder_weight, preferred_element_type=jnp.float32), "latent"
    )
    errors = rebuilt + decoder_bias[None, :] - every_token.astype(jnp.float32)
    error_grad = (LOSS_SCALE * errors).astype(jnp.bfloat16)
    back_terms = lax.dot_general(
        error_grad, decoder_weight, (((1,), (1,)), ((), ())), preferred_element_type=jnp.float32
    )
    summed = lax.psum_scatter(back_terms, "layer", scatter_dimension=1, tiled=True)
    penalty = lax.dynamic_slice_in_dim(weights_sum, offset, share_width, 0)
    grad_share = ((summed + LOSS_SCALE * SPARSITY * penalty[None, :]) * slopes).astype(jnp.bfloat16)
    pre_grad = lax.all_gather(grad_share, "layer", axis=1, tiled=True)
    encoder_grad = lax.dot_general(
        every_token, pre_grad, (((0,), (0,)), ((), ())), preferred_element_type=jnp.float32
    ).astype(jnp.bfloat16)
    totals = jnp.sum(hidden.astype(jnp.float32), axis=0)
    direct = lax.dot_general(
        hidden, error_grad, (((0,), (0,)), ((), ())), preferred_element_type=jnp.float32
    )
    sparse_term = wide * (LOSS_SCALE * SPARSITY * totals / own_norm)[:, None]
    decoder_grad = (direct + sparse_term).astype(jnp.bfloat16)
    return (encoder_grad, decoder_grad)


def call(body, out_shape, scratch, limit, flops, nbytes, args, spaces, out_spaces, aliases=None):
    out = pl.pallas_call(
        body,
        in_specs=[pl.BlockSpec(memory_space=s) for s in spaces],
        out_specs=[pl.BlockSpec(memory_space=s) for s in out_spaces],
        out_shape=out_shape,
        scratch_shapes=scratch,
        input_output_aliases=aliases or {},
        compiler_params=pltpu.CompilerParams(vmem_limit_bytes=limit * MIB),
        cost_estimate=pl.CostEstimate(flops=flops, bytes_accessed=nbytes, transcendentals=0),
    )(*args)
    return list(out)


VMEM, ANY = pltpu.VMEM, pl.ANY


def hold(weight, blocks, axis, chunk, chunks, behind, sums=None):
    shape = tuple(n // chunks if i == axis else n for i, n in enumerate(weight.shape))
    rows, wide = shape
    step = rows // blocks
    norms = sums is not None
    given = [] if not norms or isinstance(sums, str) else [sums]
    last = chunk == chunks - 1

    def body(w_hbm, *refs):
        refs = list(refs)
        given_refs = [refs.pop(0) for _ in given]
        refs = refs[len(behind) :]
        out, sems = refs[0], refs[-1]
        row, column = (chunk * rows, 0) if axis == 0 else (0, chunk * wide)
        copies = [
            pltpu.make_async_copy(
                w_hbm.at[pl.ds(row + i * step, step), pl.ds(column, wide)],
                out.at[pl.ds(i * step, step)],
                sems.at[i],
            )
            for i in range(blocks)
        ]
        for copy in copies:
            copy.start()
        for i, copy in enumerate(copies):
            copy.wait()
            if norms:
                own = slice(i * step, (i + 1) * step)
                part = jnp.zeros((step, 128), F32)
                for c in range(0, wide, 128):
                    x = out[own, c : c + 128].astype(F32)
                    part = part + x * x
                total = jnp.sum(part, axis=1, keepdims=True)
                if given:
                    total = total + given_refs[0][own, :]
                refs[1][own, :] = jnp.sqrt(total + epsilon) if last else total

    out_shape = [pltpu.VMEM(shape, weight.dtype)]
    if norms:
        out_shape.append(jax.ShapeDtypeStruct((rows, 1), F32))
    return call(
        body, out_shape, [pltpu.SemaphoreType.DMA((blocks,))], 6,
        4096 * 2048 * 128, 2 * rows * wide,
        [pltpu.with_memory_space_constraint(weight, pltpu.HBM)] + given + behind,
        [pltpu.HBM] + [VMEM] * len(given) + [ANY] * len(behind),
        [VMEM] * len(out_shape),
    )


def held(x):
    return pltpu.with_memory_space_constraint(x, pltpu.VMEM)


def encode(halves, weight, groups):
    half, wide = halves[0].shape
    rows = 2 * half
    share = weight.shape[1] // groups

    def body(a_ref, b_ref, w_ref, *refs):
        x = refs[groups]
        me = lax.axis_index("layer")
        x[:half, :] = a_ref[...]
        x[half:, :] = b_ref[...]
        for k in list(range(1, groups)) + [0]:
            at = pl.multiple_of((me ^ k) * share, share)
            y = jnp.dot(x[...], w_ref[:, pl.ds(at, share)], preferred_element_type=F32)
            refs[k][...] = y.astype(refs[k].dtype)

    kinds = [BF16 if k else F32 for k in range(groups)]
    args = [*halves, held(weight)]
    return call(
        body, [jax.ShapeDtypeStruct((rows, share), kind) for kind in kinds],
        [pltpu.VMEM((rows, wide), BF16)], 8,
        2 * rows * wide * share * groups, 2 * wide * share * groups,
        args, [VMEM] * len(args), [VMEM] * groups,
    )


def rebuild(hiddens, weights):
    groups = len(hiddens)
    rows, share = hiddens[0].shape
    half = rows // 2
    wide = weights[0].shape[1]
    total = wide * len(weights)
    block = min(512, wide)

    def body(*refs):
        hidden_refs, w_refs = refs[:groups], refs[groups : groups + len(weights)]
        keep, send, x = refs[groups + len(weights) :]
        me = lax.axis_index("layer")
        for k in range(groups):
            at = pl.multiple_of((me ^ k) * share, share)
            x[:, pl.ds(at, share)] = hidden_refs[k][...]
        for c, w_ref in enumerate(w_refs):
            for n in range(0, wide, block):
                y = jnp.dot(x[...], w_ref[:, n : n + block], preferred_element_type=F32)
                own = slice(c * wide + n, c * wide + n + block)
                keep[:, own] = y[:half]
                send[:, own] = y[half:].astype(BF16)

    args = [*hiddens] + [held(weight) for weight in weights]
    return call(
        body,
        [jax.ShapeDtypeStruct((half, total), F32), jax.ShapeDtypeStruct((half, total), BF16)],
        [pltpu.VMEM((rows, share * groups), BF16)], 8,
        2 * rows * total * share * groups, 2 * total * share * groups,
        args, [VMEM] * len(args), [VMEM] * 2,
    )


def back_product(halves, weight, norm_column, groups, acc):
    half, wide = halves[0].shape
    rows = 2 * half
    share = weight.shape[0] // groups
    last = acc is not None

    def body(a_ref, b_ref, w_ref, *refs):
        others, outs, x = refs[: groups if last else 1], refs[-1 - groups : -1], refs[-1]
        me = lax.axis_index("layer")
        x[:, :half] = a_ref[...].T
        x[:, half:] = b_ref[...].T
        for k in list(range(1, groups)) + [0]:
            at = pl.multiple_of((me ^ k) * share, share)
            y = jnp.dot(w_ref[pl.ds(at, share), :], x[...], preferred_element_type=F32)
            if last:
                y = y + others[k][...]
            else:
                y = y + (LOSS_SCALE * SPARSITY) * others[0][pl.ds(at, share), :]
            outs[k][...] = y.astype(outs[k].dtype)

    kinds = [BF16 if k and last else F32 for k in range(groups)]
    args = [*halves, held(weight)] + (acc if last else [norm_column])
    return call(
        body, [jax.ShapeDtypeStruct((share, rows), kind) for kind in kinds],
        [pltpu.VMEM((wide, rows), BF16)], 8,
        2 * rows * wide * share * groups, 2 * wide * share * groups,
        args, [VMEM] * len(args), [VMEM] * groups,
    )


def prepare(hiddens, norm_column):
    groups = len(hiddens)
    rows, share = hiddens[0].shape

    def body(*refs):
        norm_ref, turned, scale = refs[groups:]
        me = lax.axis_index("layer")
        for k in range(groups):
            h = refs[k][...].T
            at = pl.multiple_of((me ^ k) * share, share)
            own = slice(k * share, (k + 1) * share)
            totals = jnp.sum(h.astype(F32), axis=1, keepdims=True)
            turned[own, :] = h
            scale[own, :] = LOSS_SCALE * SPARSITY * totals / norm_ref[pl.ds(at, share), :]

    args = [*hiddens, norm_column]
    return call(
        body,
        [
            jax.ShapeDtypeStruct((groups * share, rows), BF16),
            jax.ShapeDtypeStruct((groups * share, 1), F32),
        ],
        [], 6, 2 * 128 * 4096 * 512, 4 * groups * share * rows, args, [VMEM] * len(args), [VMEM] * 2,
    )


def decoder_gradient(turned, scale, halves, weight, chunk, chunks, groups, into):
    latents, rows = turned.shape
    half, wide = halves[0].shape
    share = latents // groups
    step = min(256, share)
    per = share // step
    slots = 6
    block = min(1024, wide)

    def body(turned_ref, scale_ref, a_ref, b_ref, w_ref, *refs):
        out, errors, stage, sems = refs[-4:]
        me = lax.axis_index("layer")
        errors[:half, :] = a_ref[...]
        errors[half:, :] = b_ref[...]

        def place(i):
            return pl.multiple_of((me ^ (i // per)) * share + lax.rem(i, per) * step, step)

        def copy(i):
            slot = lax.rem(i, slots)
            return pltpu.make_async_copy(
                stage.at[slot],
                out.at[pl.ds(place(i), step), pl.ds(chunk * wide, wide)],
                sems.at[slot],
            )

        def loop(i, carry):
            own = pl.multiple_of(i * step, step)
            slot = lax.rem(i, slots)

            @pl.when(i >= slots)
            def _():
                copy(i - slots).wait()

            for n in range(0, wide, block):
                y = jnp.dot(
                    turned_ref[pl.ds(own, step), :], errors[:, n : n + block],
                    preferred_element_type=F32,
                )
                w = w_ref[pl.ds(place(i), step), n : n + block].astype(F32)
                stage[slot, :, n : n + block] = (
                    y + w * scale_ref[pl.ds(own, step), :]
                ).astype(BF16)
            copy(i).start()
            return carry

        trips = per * groups
        lax.fori_loop(0, trips, loop, 0)
        for i in range(max(0, trips - slots), trips):
            copy(i).wait()

    args = [turned, scale, *halves, held(weight)]
    spaces = [VMEM] * len(args)
    aliases = {}
    if into is not None:
        aliases = {len(args): 0}
        args.append(into)
        spaces.append(ANY)
    return call(
        body, [jax.ShapeDtypeStruct((latents, wide * chunks), BF16)],
        [
            pltpu.VMEM((rows, wide), BF16),
            pltpu.VMEM((slots, step, wide), BF16),
            pltpu.SemaphoreType.DMA((slots,)),
        ], 16,
        4 * rows * wide * latents, 2 * wide * latents,
        args, spaces, [ANY], aliases,
    )[0]


def activate(own, arrived, bias):
    rows, share = own.shape

    def body(own_ref, *refs):
        refs = list(refs)
        hidden_ref, slopes_ref = refs[-2:]
        preact = own_ref[...]
        for ref in refs[:-3]:
            preact = preact + ref[...].astype(F32)
        at = pl.multiple_of(lax.axis_index("layer") * share, share)
        preact = preact + refs[-3][:, pl.ds(at, share)]
        hidden_ref[...] = (jax.nn.softplus(sharpness * preact) / sharpness).astype(BF16)
        slopes_ref[...] = jax.nn.sigmoid(sharpness * preact).T

    args = [own, *arrived, bias[None, :]]
    return call(
        body,
        [jax.ShapeDtypeStruct((rows, share), BF16), jax.ShapeDtypeStruct((share, rows), F32)],
        [], 4, 2 * 128 * 4096 * 256, 12 * rows * share, args, [VMEM] * len(args), [VMEM] * 2,
    )


def split_rows(keep, arrived, places):
    half, wide = keep.shape
    rows = half // places

    def body(keep_ref, arrived_ref, *outs):
        for k, out in enumerate(outs):
            own = slice(k * rows, (k + 1) * rows)
            y = keep_ref[own, :] + arrived_ref[own, :].astype(F32)
            out[...] = y.astype(out.dtype)

    kinds = [BF16 if k else F32 for k in range(places)]
    return call(
        body, [jax.ShapeDtypeStruct((rows, wide), kind) for kind in kinds],
        [], 4, 2 * 128 * 4096 * 64, 8 * half * wide, [keep, arrived], [VMEM] * 2, [VMEM] * places,
    )


def error_value(own, arrived, bias, tokens, first):
    rows, wide = own.shape

    def body(own_ref, *refs):
        bias_ref, tokens_ref, out = refs[-3:]
        columns = slice(first, first + wide)
        value = own_ref[...]
        for ref in refs[:-3]:
            value = value + ref[...].astype(F32)
        value = value + bias_ref[:, columns] - tokens_ref[:, columns].astype(F32)
        out[...] = (LOSS_SCALE * value).astype(BF16)

    args = [own, *arrived, bias[None, :], tokens]
    return call(
        body, [jax.ShapeDtypeStruct((rows, wide), BF16)],
        [], 4, 2 * 128 * 4096 * 64, 12 * rows * wide, args, [VMEM] * len(args), [VMEM],
    )[0]


def slope_product(own, arrived, slopes):
    def body(own_ref, *refs):
        summed = own_ref[...]
        for ref in refs[:-2]:
            summed = summed + ref[...].astype(F32)
        refs[-1][...] = (summed * refs[-2][...]).astype(BF16)

    args = [own, *arrived, slopes]
    return call(
        body, [jax.ShapeDtypeStruct(own.shape, BF16)],
        [], 4, 2 * 128 * 4096 * 256, 12 * own.size, args, [VMEM] * len(args), [VMEM],
    )[0]


def turn_tokens(halves):
    half, wide = halves[0].shape

    def body(a_ref, b_ref, out):
        out[:, :half] = a_ref[...].T
        out[:, half:] = b_ref[...].T

    return call(
        body, [jax.ShapeDtypeStruct((wide, 2 * half), BF16)], [], 6,
        2 * 128 * 4096 * 512, 4 * wide * half, [*halves], [VMEM] * 2, [VMEM],
    )[0]


def encoder_gradient(gradients, ks, turned, shape, into):
    share, rows = gradients[0].shape
    count = len(ks)
    step = 1024
    per = shape[0] // step
    slots = min(8, per * count)

    def body(*rest):
        refs = list(rest)
        grad_refs = [refs.pop(0) for _ in ks]
        t_ref = refs.pop(0)
        if into is not None:
            refs.pop(0)
        out, g, stage, sems = refs
        me = lax.axis_index("layer")
        copies = []
        for i, k in enumerate(ks):
            at = pl.multiple_of((me ^ k) * share, share)
            g[...] = grad_refs[i][...].T
            for r in range(per):
                slot = len(copies) % slots
                if len(copies) >= slots:
                    copies[len(copies) - slots].wait()
                y = jnp.dot(t_ref[r * step : (r + 1) * step, :], g[...], preferred_element_type=F32)
                stage[slot] = y.astype(BF16)
                copy = pltpu.make_async_copy(
                    stage.at[slot],
                    out.at[pl.ds(r * step, step), pl.ds(at, share)],
                    sems.at[slot],
                )
                copy.start()
                copies.append(copy)
        for copy in copies[len(copies) - slots :]:
            copy.wait()

    args = [gradients[k] for k in ks] + [turned]
    spaces = [VMEM] * len(args)
    aliases = {}
    if into is not None:
        aliases = {len(args): 0}
        args.append(into)
        spaces.append(ANY)
    return call(
        body, [jax.ShapeDtypeStruct(shape, BF16)],
        [
            pltpu.VMEM((rows, share), BF16),
            pltpu.VMEM((slots, step, share), BF16),
            pltpu.SemaphoreType.DMA((slots,)),
        ], 16,
        4 * rows * shape[0] * share * count, 2 * shape[0] * share * count,
        args, spaces, [ANY], aliases,
    )[0]


def shards(tokens, encoder_weight, encoder_bias, decoder_weight, decoder_bias):
    _, width = tokens.shape
    latents = encoder_weight.shape[1]
    groups = lax.axis_size("layer")
    places = lax.axis_size("latent") // 2
    share = latents // groups
    powers = groups & (groups - 1) == 0 and places & (places - 1) == 0
    if width != D or share % 128 or width % (512 * CHUNKS) or not powers or places < 2:
        return general(tokens, encoder_weight, encoder_bias, decoder_weight, decoder_bias)

    def layer_move(x, k):
        return lax.ppermute(x, "layer", [(i, i ^ k) for i in range(groups)])

    def place_move(x, k):
        pairs = [(2 * z + c, 2 * (z ^ k) + c) for z in range(places) for c in range(2)]
        return lax.ppermute(x, "latent", pairs)

    def core_move(x):
        return lax.ppermute(x, "latent", [(i, i ^ 1) for i in range(2 * places)])

    def spread(own):
        moved = [place_move(own, k) for k in range(1, places)]
        return jnp.concatenate([own] + moved, axis=0)

    def exchange(xs):
        return [layer_move(x, k) for k, x in enumerate(xs) if k]

    encoder = hold(encoder_weight, 8, 0, 0, 1, [])[0]
    mine = spread(tokens)
    every = (mine, core_move(mine))
    acc = encode(every, encoder, groups)

    decoder, norm_column = [], "zero"
    for c in range(CHUNKS):
        held_c, norm_column = hold(
            decoder_weight, 8, 1, c, CHUNKS, [acc[1]] if c == 0 else [], norm_column
        )
        decoder.append(held_c)
    arrived = exchange(acc)
    hidden, slopes = activate(acc[0], arrived, encoder_bias)
    hiddens = [hidden] + exchange([hidden] * groups)
    turned = turn_tokens(every)
    hidden_turned, scale = prepare(hiddens, norm_column)
    piece = width // CHUNKS
    error_grads = []
    for c in range(CHUNKS):
        keep, send = rebuild(hiddens, [decoder[c]])
        parts = split_rows(keep, core_move(send), places)
        moved = [place_move(parts[k], k) for k in range(1, places)]
        value = error_value(parts[0], moved, decoder_bias, tokens, c * piece)
        mine = spread(value)
        error_grads.append((mine, core_move(mine)))
    back = None
    for c in range(CHUNKS):
        back = back_product(error_grads[c], decoder[c], norm_column, groups, back)
    arrived = exchange(back)
    grad = slope_product(back[0], arrived, slopes)
    grads = [grad] + exchange([grad] * groups)
    decoder_grad = None
    for c in range(CHUNKS):
        decoder_grad = decoder_gradient(
            hidden_turned, scale, error_grads[c], decoder[c], c, CHUNKS, groups, decoder_grad
        )
    shape = encoder_weight.shape
    encoder_grad = encoder_gradient(grads, [0], turned, shape, None)
    encoder_grad = encoder_gradient(
        grads, list(range(1, groups)), turned, shape, encoder_grad
    )
    return (encoder_grad, decoder_grad)


def solution(mesh):
    placed = (
        P("latent", "layer"),
        P("layer", "latent"),
        P("latent"),
        P("latent", "layer"),
        P("layer"),
    )

    return jax.shard_map(
        shards,
        mesh=mesh,
        in_specs=placed,
        out_specs=(P("layer", "latent"), P("latent", "layer")),
        check_vma=False,
    )
```

```python
import jax
import jax.numpy as jnp
from jax import lax
from jax.experimental import pallas as pl
from jax.experimental.pallas import tpu as pltpu
from jax.sharding import PartitionSpec as P


L = 4
D = 4096


LOSS_SCALE = 0.0625
SPARSITY = 0.5
sharpness = 4.0
epsilon = 1e-06


CHUNKS = 2
F32 = jnp.float32
BF16 = jnp.bfloat16
MIB = 1024 * 1024


def general(tokens, encoder_weight, encoder_bias, decoder_weight, decoder_bias):
    _, width_dev = tokens.shape
    latents_dev = encoder_weight.shape[1]
    groups = lax.axis_size("layer")
    layer_index = lax.axis_index("layer") * width_dev // D
    wide = decoder_weight.astype(jnp.float32)
    squares_own = jnp.sum(wide * wide, axis=1)
    placed = jnp.where(jnp.arange(L)[:, None] == layer_index, squares_own[None, :], 0.0)
    squares = lax.psum(placed, "layer")
    row_norms = jnp.sqrt(squares + epsilon)
    weights_sum = jnp.sum(row_norms, axis=0)
    own_norm = lax.dynamic_slice_in_dim(row_norms, layer_index, 1, 0)[0]
    every_token = lax.all_gather(tokens, "latent", axis=0, tiled=True)
    partial_value = jnp.dot(every_token, encoder_weight, preferred_element_type=jnp.float32)
    share_width = latents_dev // groups
    offset = lax.axis_index("layer") * share_width
    preact = lax.psum_scatter(partial_value, "layer", scatter_dimension=1, tiled=True)
    preact = preact + lax.dynamic_slice_in_dim(encoder_bias, offset, share_width, 0)[None, :]
    hidden_share = (jax.nn.softplus(sharpness * preact) / sharpness).astype(jnp.bfloat16)
    hidden = lax.all_gather(hidden_share, "layer", axis=1, tiled=True)
    slopes = jax.nn.sigmoid(sharpness * preact)
    rebuilt = lax.psum(
        jnp.dot(hidden, decoder_weight, preferred_element_type=jnp.float32), "latent"
    )
    errors = rebuilt + decoder_bias[None, :] - every_token.astype(jnp.float32)
    error_grad = (LOSS_SCALE * errors).astype(jnp.bfloat16)
    back_terms = lax.dot_general(
        error_grad, decoder_weight, (((1,), (1,)), ((), ())), preferred_element_type=jnp.float32
    )
    summed = lax.psum_scatter(back_terms, "layer", scatter_dimension=1, tiled=True)
    penalty = lax.dynamic_slice_in_dim(weights_sum, offset, share_width, 0)
    grad_share = ((summed + LOSS_SCALE * SPARSITY * penalty[None, :]) * slopes).astype(jnp.bfloat16)
    pre_grad = lax.all_gather(grad_share, "layer", axis=1, tiled=True)
    encoder_grad = lax.dot_general(
        every_token, pre_grad, (((0,), (0,)), ((), ())), preferred_element_type=jnp.float32
    ).astype(jnp.bfloat16)
    totals = jnp.sum(hidden.astype(jnp.float32), axis=0)
    direct = lax.dot_general(
        hidden, error_grad, (((0,), (0,)), ((), ())), preferred_element_type=jnp.float32
    )
    sparse_term = wide * (LOSS_SCALE * SPARSITY * totals / own_norm)[:, None]
    decoder_grad = (direct + sparse_term).astype(jnp.bfloat16)
    return (encoder_grad, decoder_grad)


def call(body, out_shape, scratch, limit, flops, nbytes, args, spaces, out_spaces, aliases=None):
    out = pl.pallas_call(
        body,
        in_specs=[pl.BlockSpec(memory_space=s) for s in spaces],
        out_specs=[pl.BlockSpec(memory_space=s) for s in out_spaces],
        out_shape=out_shape,
        scratch_shapes=scratch,
        input_output_aliases=aliases or {},
        compiler_params=pltpu.CompilerParams(vmem_limit_bytes=limit * MIB),
        cost_estimate=pl.CostEstimate(flops=flops, bytes_accessed=nbytes, transcendentals=0),
    )(*args)
    return list(out)


VMEM, ANY = pltpu.VMEM, pl.ANY


def hold(weight, blocks, axis, chunk, chunks, behind, sums=None):
    shape = tuple(n // chunks if i == axis else n for i, n in enumerate(weight.shape))
    rows, wide = shape
    step = rows // blocks
    norms = sums is not None
    given = [] if not norms or isinstance(sums, str) else [sums]
    last = chunk == chunks - 1

    def body(w_hbm, *refs):
        refs = list(refs)
        given_refs = [refs.pop(0) for _ in given]
        refs = refs[len(behind) :]
        out, sems = refs[0], refs[-1]
        row, column = (chunk * rows, 0) if axis == 0 else (0, chunk * wide)
        copies = [
            pltpu.make_async_copy(
                w_hbm.at[pl.ds(row + i * step, step), pl.ds(column, wide)],
                out.at[pl.ds(i * step, step)],
                sems.at[i],
            )
            for i in range(blocks)
        ]
        for copy in copies:
            copy.start()
        for i, copy in enumerate(copies):
            copy.wait()
            if norms:
                own = slice(i * step, (i + 1) * step)
                part = jnp.zeros((step, 128), F32)
                for c in range(0, wide, 128):
                    x = out[own, c : c + 128].astype(F32)
                    part = part + x * x
                total = jnp.sum(part, axis=1, keepdims=True)
                if given:
                    total = total + given_refs[0][own, :]
                refs[1][own, :] = jnp.sqrt(total + epsilon) if last else total

    out_shape = [pltpu.VMEM(shape, weight.dtype)]
    if norms:
        out_shape.append(jax.ShapeDtypeStruct((rows, 1), F32))
    return call(
        body, out_shape, [pltpu.SemaphoreType.DMA((blocks,))], 6,
        4096 * 2048 * 128, 2 * rows * wide,
        [pltpu.with_memory_space_constraint(weight, pltpu.HBM)] + given + behind,
        [pltpu.HBM] + [VMEM] * len(given) + [ANY] * len(behind),
        [VMEM] * len(out_shape),
    )


def held(x):
    return pltpu.with_memory_space_constraint(x, pltpu.VMEM)


def encode(halves, weight, groups, ks):
    half, wide = halves[0].shape
    rows = 2 * half
    share = weight.shape[1] // groups

    def body(a_ref, b_ref, w_ref, *refs):
        x = refs[-1]
        me = lax.axis_index("layer")
        x[:half, :] = a_ref[...]
        x[half:, :] = b_ref[...]
        for out, k in zip(refs, ks):
            at = pl.multiple_of((me ^ k) * share, share)
            y = jnp.dot(x[...], w_ref[:, pl.ds(at, share)], preferred_element_type=F32)
            out[...] = y.astype(out.dtype)

    kinds = [BF16 if k else F32 for k in ks]
    args = [*halves, held(weight)]
    return call(
        body, [jax.ShapeDtypeStruct((rows, share), kind) for kind in kinds],
        [pltpu.VMEM((rows, wide), BF16)], 8,
        2 * rows * wide * share * len(ks), 2 * wide * share * len(ks),
        args, [VMEM] * len(args), [VMEM] * len(ks),
    )


def rebuild(hiddens, weights):
    groups = len(hiddens)
    rows, share = hiddens[0].shape
    half = rows // 2
    wide = weights[0].shape[1]
    total = wide * len(weights)
    block = min(512, wide)

    def body(*refs):
        hidden_refs, w_refs = refs[:groups], refs[groups : groups + len(weights)]
        keep, send, x = refs[groups + len(weights) :]
        me = lax.axis_index("layer")
        for k in range(groups):
            at = pl.multiple_of((me ^ k) * share, share)
            x[:, pl.ds(at, share)] = hidden_refs[k][...]
        for c, w_ref in enumerate(w_refs):
            for n in range(0, wide, block):
                y = jnp.dot(x[...], w_ref[:, n : n + block], preferred_element_type=F32)
                own = slice(c * wide + n, c * wide + n + block)
                keep[:, own] = y[:half]
                send[:, own] = y[half:].astype(BF16)

    args = [*hiddens] + [held(weight) for weight in weights]
    return call(
        body,
        [jax.ShapeDtypeStruct((half, total), F32), jax.ShapeDtypeStruct((half, total), BF16)],
        [pltpu.VMEM((rows, share * groups), BF16)], 8,
        2 * rows * total * share * groups, 2 * total * share * groups,
        args, [VMEM] * len(args), [VMEM] * 2,
    )


def back_product(halves, weight, norm_column, groups, acc):
    half, wide = halves[0].shape
    rows = 2 * half
    share = weight.shape[0] // groups
    last = acc is not None

    def body(a_ref, b_ref, w_ref, *refs):
        others, outs, x = refs[: groups if last else 1], refs[-1 - groups : -1], refs[-1]
        me = lax.axis_index("layer")
        x[:, :half] = a_ref[...].T
        x[:, half:] = b_ref[...].T
        for k in list(range(1, groups)) + [0]:
            at = pl.multiple_of((me ^ k) * share, share)
            y = jnp.dot(w_ref[pl.ds(at, share), :], x[...], preferred_element_type=F32)
            if last:
                y = y + others[k][...]
            else:
                y = y + (LOSS_SCALE * SPARSITY) * others[0][pl.ds(at, share), :]
            outs[k][...] = y.astype(outs[k].dtype)

    kinds = [BF16 if k and last else F32 for k in range(groups)]
    args = [*halves, held(weight)] + (acc if last else [norm_column])
    return call(
        body, [jax.ShapeDtypeStruct((share, rows), kind) for kind in kinds],
        [pltpu.VMEM((wide, rows), BF16)], 8,
        2 * rows * wide * share * groups, 2 * wide * share * groups,
        args, [VMEM] * len(args), [VMEM] * groups,
    )


def prepare(hiddens, norm_column):
    groups = len(hiddens)
    rows, share = hiddens[0].shape

    def body(*refs):
        norm_ref, turned, scale = refs[groups:]
        me = lax.axis_index("layer")
        for k in range(groups):
            h = refs[k][...].T
            at = pl.multiple_of((me ^ k) * share, share)
            own = slice(k * share, (k + 1) * share)
            totals = jnp.sum(h.astype(F32), axis=1, keepdims=True)
            turned[own, :] = h
            scale[own, :] = LOSS_SCALE * SPARSITY * totals / norm_ref[pl.ds(at, share), :]

    args = [*hiddens, norm_column]
    return call(
        body,
        [
            jax.ShapeDtypeStruct((groups * share, rows), BF16),
            jax.ShapeDtypeStruct((groups * share, 1), F32),
        ],
        [], 6, 2 * 128 * 4096 * 512, 4 * groups * share * rows, args, [VMEM] * len(args), [VMEM] * 2,
    )


def decoder_gradient(turned, scale, halves, weight, chunk, chunks, groups, ks, into):
    latents, rows = turned.shape
    half, wide = halves[0].shape
    share = latents // groups
    step = min(256, share)
    per = share // step
    begin, end = per * ks[0], per * (ks[-1] + 1)
    slots = min(6, end - begin)
    block = min(1024, wide)

    def body(turned_ref, scale_ref, a_ref, b_ref, w_ref, *refs):
        out, errors, stage, sems = refs[-4:]
        me = lax.axis_index("layer")
        errors[:half, :] = a_ref[...]
        errors[half:, :] = b_ref[...]

        def place(i):
            return pl.multiple_of((me ^ (i // per)) * share + lax.rem(i, per) * step, step)

        def copy(i):
            slot = lax.rem(i, slots)
            return pltpu.make_async_copy(
                stage.at[slot],
                out.at[pl.ds(place(i), step), pl.ds(chunk * wide, wide)],
                sems.at[slot],
            )

        def loop(i, carry):
            own = pl.multiple_of(i * step, step)
            slot = lax.rem(i, slots)

            @pl.when(i >= begin + slots)
            def _():
                copy(i - slots).wait()

            for n in range(0, wide, block):
                y = jnp.dot(
                    turned_ref[pl.ds(own, step), :], errors[:, n : n + block],
                    preferred_element_type=F32,
                )
                w = w_ref[pl.ds(place(i), step), n : n + block].astype(F32)
                stage[slot, :, n : n + block] = (
                    y + w * scale_ref[pl.ds(own, step), :]
                ).astype(BF16)
            copy(i).start()
            return carry

        lax.fori_loop(begin, end, loop, 0, unroll=True)
        for i in range(end - slots, end):
            copy(i).wait()

    args = [turned, scale, *halves, held(weight)]
    spaces = [VMEM] * len(args)
    aliases = {}
    if into is not None:
        aliases = {len(args): 0}
        args.append(into)
        spaces.append(ANY)
    return call(
        body, [jax.ShapeDtypeStruct((latents, wide * chunks), BF16)],
        [
            pltpu.VMEM((rows, wide), BF16),
            pltpu.VMEM((slots, step, wide), BF16),
            pltpu.SemaphoreType.DMA((slots,)),
        ], 16,
        4 * rows * wide * share * len(ks), 2 * wide * share * len(ks),
        args, spaces, [ANY], aliases,
    )[0]


def activate(own, arrived, bias):
    rows, share = own.shape

    def body(own_ref, *refs):
        refs = list(refs)
        hidden_ref, slopes_ref = refs[-2:]
        preact = own_ref[...]
        for ref in refs[:-3]:
            preact = preact + ref[...].astype(F32)
        at = pl.multiple_of(lax.axis_index("layer") * share, share)
        preact = preact + refs[-3][:, pl.ds(at, share)]
        hidden_ref[...] = (jax.nn.softplus(sharpness * preact) / sharpness).astype(BF16)
        slopes_ref[...] = jax.nn.sigmoid(sharpness * preact).T

    args = [own, *arrived, bias[None, :]]
    return call(
        body,
        [jax.ShapeDtypeStruct((rows, share), BF16), jax.ShapeDtypeStruct((share, rows), F32)],
        [], 4, 2 * 128 * 4096 * 256, 12 * rows * share, args, [VMEM] * len(args), [VMEM] * 2,
    )


def split_rows(keep, arrived, places):
    half, wide = keep.shape
    rows = half // places

    def body(keep_ref, arrived_ref, *outs):
        for k, out in enumerate(outs):
            own = slice(k * rows, (k + 1) * rows)
            y = keep_ref[own, :] + arrived_ref[own, :].astype(F32)
            out[...] = y.astype(out.dtype)

    kinds = [BF16 if k else F32 for k in range(places)]
    return call(
        body, [jax.ShapeDtypeStruct((rows, wide), kind) for kind in kinds],
        [], 4, 2 * 128 * 4096 * 64, 8 * half * wide, [keep, arrived], [VMEM] * 2, [VMEM] * places,
    )


def error_value(own, arrived, bias, tokens, first):
    rows, wide = own.shape

    def body(own_ref, *refs):
        bias_ref, tokens_ref, out = refs[-3:]
        columns = slice(first, first + wide)
        value = own_ref[...]
        for ref in refs[:-3]:
            value = value + ref[...].astype(F32)
        value = value + bias_ref[:, columns] - tokens_ref[:, columns].astype(F32)
        out[...] = (LOSS_SCALE * value).astype(BF16)

    args = [own, *arrived, bias[None, :], tokens]
    return call(
        body, [jax.ShapeDtypeStruct((rows, wide), BF16)],
        [], 4, 2 * 128 * 4096 * 64, 12 * rows * wide, args, [VMEM] * len(args), [VMEM],
    )[0]


def slope_product(own, arrived, slopes):
    def body(own_ref, *refs):
        summed = own_ref[...]
        for ref in refs[:-2]:
            summed = summed + ref[...].astype(F32)
        refs[-1][...] = (summed * refs[-2][...]).astype(BF16)

    args = [own, *arrived, slopes]
    return call(
        body, [jax.ShapeDtypeStruct(own.shape, BF16)],
        [], 4, 2 * 128 * 4096 * 256, 12 * own.size, args, [VMEM] * len(args), [VMEM],
    )[0]


def turn_tokens(halves):
    half, wide = halves[0].shape

    def body(a_ref, b_ref, out):
        out[:, :half] = a_ref[...].T
        out[:, half:] = b_ref[...].T

    return call(
        body, [jax.ShapeDtypeStruct((wide, 2 * half), BF16)], [], 6,
        2 * 128 * 4096 * 512, 4 * wide * half, [*halves], [VMEM] * 2, [VMEM],
    )[0]


def encoder_gradient(gradients, ks, turned, shape, into):
    share, rows = gradients[0].shape
    count = len(ks)
    step = 1024
    per = shape[0] // step
    slots = min(8, per * count)

    def body(*rest):
        refs = list(rest)
        grad_refs = [refs.pop(0) for _ in ks]
        t_ref = refs.pop(0)
        if into is not None:
            refs.pop(0)
        out, g, stage, sems = refs
        me = lax.axis_index("layer")
        copies = []
        for i, k in enumerate(ks):
            at = pl.multiple_of((me ^ k) * share, share)
            g[...] = grad_refs[i][...].T
            for r in range(per):
                slot = len(copies) % slots
                if len(copies) >= slots:
                    copies[len(copies) - slots].wait()
                y = jnp.dot(t_ref[r * step : (r + 1) * step, :], g[...], preferred_element_type=F32)
                stage[slot] = y.astype(BF16)
                copy = pltpu.make_async_copy(
                    stage.at[slot],
                    out.at[pl.ds(r * step, step), pl.ds(at, share)],
                    sems.at[slot],
                )
                copy.start()
                copies.append(copy)
        for copy in copies[len(copies) - slots :]:
            copy.wait()

    args = [gradients[k] for k in ks] + [turned]
    spaces = [VMEM] * len(args)
    aliases = {}
    if into is not None:
        aliases = {len(args): 0}
        args.append(into)
        spaces.append(ANY)
    return call(
        body, [jax.ShapeDtypeStruct(shape, BF16)],
        [
            pltpu.VMEM((rows, share), BF16),
            pltpu.VMEM((slots, step, share), BF16),
            pltpu.SemaphoreType.DMA((slots,)),
        ], 16,
        4 * rows * shape[0] * share * count, 2 * shape[0] * share * count,
        args, spaces, [ANY], aliases,
    )[0]


def shards(tokens, encoder_weight, encoder_bias, decoder_weight, decoder_bias):
    _, width = tokens.shape
    latents = encoder_weight.shape[1]
    groups = lax.axis_size("layer")
    places = lax.axis_size("latent") // 2
    share = latents // groups
    powers = groups & (groups - 1) == 0 and places & (places - 1) == 0
    if width != D or share % 128 or width % (512 * CHUNKS) or not powers or places < 2:
        return general(tokens, encoder_weight, encoder_bias, decoder_weight, decoder_bias)

    def layer_move(x, k):
        return lax.ppermute(x, "layer", [(i, i ^ k) for i in range(groups)])

    def place_move(x, k):
        pairs = [(2 * z + c, 2 * (z ^ k) + c) for z in range(places) for c in range(2)]
        return lax.ppermute(x, "latent", pairs)

    def core_move(x):
        return lax.ppermute(x, "latent", [(i, i ^ 1) for i in range(2 * places)])

    def spread(own):
        moved = [place_move(own, k) for k in range(1, places)]
        return jnp.concatenate([own] + moved, axis=0)

    def exchange(xs, first=0):
        return [layer_move(x, k) for k, x in enumerate(xs, first) if k]

    encoder = hold(encoder_weight, 8, 0, 0, 1, [])[0]
    mine = spread(tokens)
    every = (mine, core_move(mine))
    half = groups // 2
    acc = encode(every, encoder, groups, list(range(half, groups)))
    acc = encode(every, encoder, groups, list(range(half))) + acc

    decoder, norm_column = [], "zero"
    for c in range(CHUNKS):
        held_c, norm_column = hold(
            decoder_weight, 8, 1, c, CHUNKS, [acc[1]] if c == 0 else [], norm_column
        )
        decoder.append(held_c)
    arrived = exchange(acc[:half]) + exchange(acc[half:], half)
    hidden, slopes = activate(acc[0], arrived, encoder_bias)
    hiddens = [hidden] + exchange([hidden] * groups)
    turned = turn_tokens(every)
    hidden_turned, scale = prepare(hiddens, norm_column)
    piece = width // CHUNKS
    error_grads = []
    for c in range(CHUNKS):
        keep, send = rebuild(hiddens, [decoder[c]])
        parts = split_rows(keep, core_move(send), places)
        moved = [place_move(parts[k], k) for k in range(1, places)]
        value = error_value(parts[0], moved, decoder_bias, tokens, c * piece)
        mine = spread(value)
        error_grads.append((mine, core_move(mine)))
    back = None
    for c in range(CHUNKS):
        back = back_product(error_grads[c], decoder[c], norm_column, groups, back)
    arrived = exchange(back)
    grad = slope_product(back[0], arrived, slopes)
    grads = [grad] + exchange([grad] * groups)
    decoder_grad = None
    pieces = [(c, range(groups)) for c in range(CHUNKS - 1)]
    pieces += [(CHUNKS - 1, range(half)), (CHUNKS - 1, range(half, groups))]
    for c, ks in pieces:
        decoder_grad = decoder_gradient(
            hidden_turned, scale, error_grads[c], decoder[c], c, CHUNKS, groups, list(ks),
            decoder_grad,
        )
    shape = encoder_weight.shape
    encoder_grad = encoder_gradient(grads, [0], turned, shape, None)
    encoder_grad = encoder_gradient(
        grads, list(range(1, groups)), turned, shape, encoder_grad
    )
    return (encoder_grad, decoder_grad)


def solution(mesh):
    placed = (
        P("latent", "layer"),
        P("layer", "latent"),
        P("latent"),
        P("latent", "layer"),
        P("layer"),
    )

    return jax.shard_map(
        shards,
        mesh=mesh,
        in_specs=placed,
        out_specs=(P("layer", "latent"), P("latent", "layer")),
        check_vma=False,
    )
```
